8 devices in a mesh: dp: 1 (over z), tp: 2 (over y), sp: 4 (over x, core).
Axes of the slice: x: 2, y: 2, z: 1, core: 2. Of those that a mesh axis runs over, the one named last changes fastest.
Arguments:
- x_tokens: bfloat16 [2048, 4096], P(('dp', 'sp'), 'tp')
- doc_ids: int32 [2048], P(('dp', 'sp'))
- w_qkv: bfloat16 [4096, 12288], P('sp', 'tp')
- w_out: bfloat16 [4096, 4096], P('sp', 'tp')
Outputs:
- output: bfloat16 [2048, 4096], P(('dp', 'sp', 'tp'))
All inputs are finite; a program needn't handle non-finite values.
Results may differ from the reference program's by a relative error of at most 0.00248.
Values are sent between devices in bfloat16 or wider.
A program may use at most 1 GiB of HBM per device.

```python
import jax
import jax.numpy as jnp
from jax import lax

SEQ_LEN = 2048
HIDDEN = 4096
NUM_HEADS = 32
HEAD_DIM = 128
QUERY_BLOCK = 512
NUM_PIECES = 32
NUM_CUTS = 3

NUM_QBLOCKS = SEQ_LEN // QUERY_BLOCK
PIECE_LEN = SEQ_LEN // NUM_PIECES
SOFTMAX_SCALE = HEAD_DIM ** -0.5


def draw_segments(seg_key):
    cut_points = jax.random.randint(seg_key, (NUM_CUTS,), 1, SEQ_LEN)
    positions = jnp.arange(SEQ_LEN, dtype=jnp.int32)
    return jnp.sum((positions[:, None] >= cut_points[None, :]).astype(jnp.int32), axis=1).astype(jnp.int32)


def setup_inputs(seed: int = 0, part: int = 0) -> dict:
    base_key = jax.random.key(seed)
    part_key = jax.random.fold_in(base_key, part)
    noise_key, piece_key, seg_key = jax.random.split(part_key, 3)
    wqkv_key, wout_key = jax.random.split(jax.random.key(seed + 1), 2)
    x_noise = jax.random.normal(noise_key, (NUM_PIECES, PIECE_LEN, HIDDEN), jnp.float32)
    pieces = jax.random.normal(piece_key, (NUM_PIECES, 1, HIDDEN), jnp.float32)
    x_val = 0.6 * x_noise + 0.8 * pieces
    x_tokens = x_val.reshape(SEQ_LEN, HIDDEN).astype(jnp.bfloat16)
    w_qkv = (jax.random.normal(wqkv_key, (HIDDEN, 3 * HIDDEN), jnp.float32) * HIDDEN ** -0.5).astype(jnp.bfloat16)
    w_out = (jax.random.normal(wout_key, (HIDDEN, HIDDEN), jnp.float32) * (2.0 * HIDDEN ** -0.5)).astype(jnp.bfloat16)
    return {"x_tokens": x_tokens, "doc_ids": draw_segments(seg_key), "w_qkv": w_qkv, "w_out": w_out}


def reference(x_tokens, doc_ids, w_qkv, w_out):
    qkv_all = jnp.dot(x_tokens, w_qkv, preferred_element_type=jnp.float32).astype(jnp.bfloat16)
    per_head = qkv_all.reshape(SEQ_LEN, NUM_HEADS, 3, HEAD_DIM).transpose(1, 2, 0, 3).astype(jnp.float32)
    doc_blocks = doc_ids.reshape(NUM_QBLOCKS, QUERY_BLOCK)

    def head_attention(head_qkv):
        key_head = head_qkv[1]
        value_head = head_qkv[2]
        query_blocks = head_qkv[0].reshape(NUM_QBLOCKS, QUERY_BLOCK, HEAD_DIM)

        def block_attention(block):
            query_blk, doc_blk = block
            scores = jnp.dot(query_blk, key_head.T, preferred_element_type=jnp.float32) * SOFTMAX_SCALE
            same_doc = doc_blk[:, None] == doc_ids[None, :]
            scores = jnp.where(same_doc, scores, -jnp.inf)
            weights = jax.nn.softmax(scores, axis=-1).astype(jnp.bfloat16).astype(jnp.float32)
            return jnp.dot(weights, value_head, preferred_element_type=jnp.float32)

        context = lax.map(block_attention, (query_blocks, doc_blocks))
        return context.reshape(SEQ_LEN, HEAD_DIM).astype(jnp.bfloat16)

    context_all = lax.map(head_attention, per_head)
    context_all = context_all.transpose(1, 0, 2).reshape(SEQ_LEN, HIDDEN)
    return jnp.dot(context_all, w_out, preferred_element_type=jnp.float32).astype(jnp.bfloat16)
```

```python
import functools

import jax
import jax.numpy as jnp
from jax import lax
from jax.experimental import pallas as pl
from jax.experimental.pallas import tpu as pltpu
from jax.sharding import PartitionSpec as P

HEAD_DIM = 128
SOFTMAX_SCALE = HEAD_DIM ** -0.5
TRIPLE = 3 * HEAD_DIM
SP = 4
TP = 2


def block_kernel(
    x_ref, doc_ref, wqkv_ref, wout_ref, y_ref,
    x_all, w_all, wo_all, o_all, o_own, qkv, y_buf, doc_all, doc_col,
    local_sem, w_local_sem, x_send, x_recv, doc_send, doc_recv, w_send, w_recv,
    wo_local_sem, wo_send, wo_recv, o_send, o_recv, of_send, of_recv, y_send, y_recv, y_local_sem,
):
    me = lax.axis_index("sp")
    col = lax.axis_index("tp")
    rows, half = x_ref.shape
    depth = wqkv_ref.shape[0]
    heads = w_all.shape[0]
    chunks = y_buf.shape[0]
    width = y_buf.shape[2]
    other_col = 1 - col
    chip = me // 2
    core = lax.rem(me, 2)
    mate = chip * 2 + 1 - core
    across = (1 - chip) * 2 + core
    diagonal = (1 - chip) * 2 + 1 - core
    peers = (mate, across, diagonal)

    barrier = pltpu.get_barrier_semaphore()
    for peer in peers:
        pl.semaphore_signal(barrier, inc=1, device_id={"sp": peer}, device_id_type=pl.DeviceIdType.MESH)
    pl.semaphore_signal(barrier, inc=1, device_id={"tp": other_col}, device_id_type=pl.DeviceIdType.MESH)
    pl.semaphore_wait(barrier, 4)

    def remote(src, dst, send, recv, where):
        return pltpu.make_async_remote_copy(
            src_ref=src, dst_ref=dst, send_sem=send, recv_sem=recv,
            device_id=where, device_id_type=pl.DeviceIdType.MESH,
        )

    def x_slot(c, s):
        return x_all.at[c, pl.ds(pl.multiple_of(s * rows, rows), rows), :]

    def x_copy(i, c, s, where, src=None):
        slot = x_slot(c, s)
        return remote(slot if src is None else src, slot, x_send.at[i], x_recv.at[i], where)

    to_mate, to_across, to_col = {"sp": mate}, {"sp": across}, {"tp": other_col}

    x_sends = [
        x_copy(0, col, me, to_mate, x_ref),
        x_copy(1, col, me, to_across, x_ref),
        x_copy(2, col, me, to_col, x_ref),
    ]
    for copy in x_sends:
        copy.start()
    x_local = pltpu.make_async_copy(x_ref, x_slot(col, me), local_sem.at[0])
    x_local.start()
    doc_local = pltpu.make_async_copy(doc_ref, doc_all.at[me], local_sem.at[1])
    doc_local.start()
    doc_sends = []
    for i, peer in enumerate(peers):
        copy = remote(doc_ref, doc_all.at[me], doc_send.at[i], doc_recv.at[i], {"sp": peer})
        copy.start()
        doc_sends.append(copy)

    def w_cols(owner, h):
        start = pl.multiple_of((owner * heads + h) * TRIPLE, TRIPLE)
        return wqkv_ref.at[:, pl.ds(start, TRIPLE)]

    def w_slot(h, s):
        return w_all.at[h, pl.ds(pl.multiple_of(s * depth, depth), depth), :]

    def w_copy(i, h):
        return remote(w_cols(peers[i], h), w_slot(h, me), w_send.at[h, i], w_recv.at[h, i], {"sp": peers[i]})

    def w_local(h):
        return pltpu.make_async_copy(w_cols(me, h), w_slot(h, me), w_local_sem.at[h])

    for h in range(heads):
        w_copy(1, h).start()
        w_copy(2, h).start()
        w_copy(0, h).start()
        w_local(h).start()

    def wo_cols(j):
        return pl.ds(pl.multiple_of(j * width, width), width)

    def wo_slot(s, j):
        return wo_all.at[pl.ds(pl.multiple_of(s * depth, depth), depth), wo_cols(j)]

    wo_local = pltpu.make_async_copy(wout_ref, wo_all.at[pl.ds(pl.multiple_of(me * depth, depth), depth), :], wo_local_sem)
    wo_local.start()

    x_copy(2, other_col, me, to_col).wait_recv()
    x_sends.append(x_copy(5, other_col, me, to_mate))
    x_sends[-1].start()
    x_copy(1, col, across, to_across).wait_recv()
    x_sends.append(x_copy(4, col, across, to_col))
    x_sends[-1].start()
    x_sends.append(x_copy(3, col, across, to_mate))
    x_sends[-1].start()

    doc_local.wait()
    for i, peer in enumerate(peers):
        remote(doc_ref, doc_all.at[peer], doc_send.at[i], doc_recv.at[i], {"sp": peer}).wait_recv()
    for s in range(SP):
        tall = jnp.broadcast_to(doc_all[s], (HEAD_DIM, rows))
        doc_col[pl.ds(s * rows, rows), :] = tall.T

    x_copy(4, other_col, across, to_col).wait_recv()
    x_sends.append(x_copy(6, other_col, across, to_mate))
    x_sends[-1].start()
    x_local.wait()
    x_copy(0, col, mate, to_mate).wait_recv()
    x_copy(3, col, diagonal, to_mate).wait_recv()
    x_copy(5, other_col, mate, to_mate).wait_recv()
    x_copy(6, other_col, diagonal, to_mate).wait_recv()

    def wo_to_mate(j):
        return remote(wout_ref.at[:, wo_cols(j)], wo_slot(me, j), wo_send.at[0, j], wo_recv.at[0, j], to_mate)

    def wo_to_across(j):
        return remote(wout_ref.at[:, wo_cols(j)], wo_slot(me, j), wo_send.at[1, j], wo_recv.at[1, j], to_across)

    def wo_pass(j):
        slot = wo_slot(across, j)
        return remote(slot, slot, wo_send.at[2, j], wo_recv.at[2, j], to_mate)

    def o_slot(c, s, h):
        return o_all.at[c, s, :, pl.ds(pl.multiple_of(h * HEAD_DIM, HEAD_DIM), HEAD_DIM)]

    def o_copy(i, h):
        src = o_own.at[h, pl.ds(pl.multiple_of(peers[i] * rows, rows), rows), :]
        return remote(src, o_slot(col, me, h), o_send.at[h, i], o_recv.at[h, i], {"sp": peers[i]})

    def o_pass(h):
        slot = o_all.at[col, :, :, pl.ds(pl.multiple_of(h * HEAD_DIM, HEAD_DIM), HEAD_DIM)]
        return remote(slot, slot, of_send.at[h], of_recv.at[h], to_col)

    def o_collect(h):
        for i in range(3):
            remote(o_slot(col, peers[i], h), o_slot(col, peers[i], h), o_send.at[h, i], o_recv.at[h, i], {"sp": peers[i]}).wait_recv()
        o_pass(h).start()

    early = chunks // 2

    def one_head(h, carry):
        w_local(h).wait()
        for i in range(3):
            remote(w_cols(peers[i], h), w_slot(h, peers[i]), w_send.at[h, i], w_recv.at[h, i], {"sp": peers[i]}).wait_recv()

        @pl.when(h == heads - 2)
        def _():
            for j in range(early):
                wo_to_across(j).start()

        def project(r, carry):
            tile = pl.ds(pl.multiple_of(r * rows, rows), rows)
            total = jnp.dot(x_all[0, tile, :], w_all[h, :half, :], preferred_element_type=jnp.float32)
            total += jnp.dot(x_all[1, tile, :], w_all[h, half:, :], preferred_element_type=jnp.float32)
            qkv[tile, :] = total.astype(jnp.bfloat16)
            return carry

        lax.fori_loop(0, SP, project, 0)

        docs = jnp.concatenate([doc_all[s] for s in range(SP)], axis=1)

        def attend(r, carry):
            tile = pl.ds(pl.multiple_of(r * 256, 256), 256)
            query = qkv[tile, :HEAD_DIM]
            scores = lax.dot_general(
                query, qkv[:, HEAD_DIM:2 * HEAD_DIM], (((1,), (1,)), ((), ())),
                preferred_element_type=jnp.float32,
            ) * SOFTMAX_SCALE
            same = doc_col[tile, :1] == docs
            scores = jnp.where(same, scores, -jnp.inf)
            top = jnp.max(scores, axis=1, keepdims=True)
            weights = jnp.exp(scores - top)
            weights = weights * (1.0 / jnp.sum(weights, axis=1, keepdims=True))
            out = jnp.dot(weights.astype(jnp.bfloat16), qkv[:, 2 * HEAD_DIM:], preferred_element_type=jnp.float32)
            o_own[h, tile, :] = out.astype(jnp.bfloat16)
            return carry

        lax.fori_loop(0, SP * rows // 256, attend, 0)
        mine = pl.ds(pl.multiple_of(me * rows, rows), rows)
        o_all[col, me, :, pl.ds(pl.multiple_of(h * HEAD_DIM, HEAD_DIM), HEAD_DIM)] = o_own[h, mine, :]
        for i in (1, 2, 0):
            o_copy(i, h).start()

        @pl.when(h >= 1)
        def _():
            o_collect(h - 1)

        return carry

    lax.fori_loop(0, heads, one_head, 0)
    for j in range(early, chunks):
        wo_to_across(j).start()
    for j in range(chunks):
        wo_to_mate(j).start()
    wo_local.wait()
    o_collect(heads - 1)

    def other_half(h):
        slot = o_all.at[other_col, :, :, pl.ds(pl.multiple_of(h * HEAD_DIM, HEAD_DIM), HEAD_DIM)]
        return remote(slot, slot, of_send.at[h], of_recv.at[h], to_col)

    keep = pl.ds(pl.multiple_of(col * (rows // 2), rows // 2), rows // 2)
    give = pl.ds(pl.multiple_of(other_col * (rows // 2), rows // 2), rows // 2)

    def y_cols(c, j):
        return pl.ds(pl.multiple_of(c * (chunks * width) + j * width, width), width)

    def y_copy(j):
        return remote(y_buf.at[j, give, :], y_ref.at[:, y_cols(col, j)], y_send.at[j], y_recv.at[j], to_col)

    def y_local(j):
        return pltpu.make_async_copy(y_buf.at[j, keep, :], y_ref.at[:, y_cols(col, j)], y_local_sem.at[j])

    def y_arrive(j):
        return remote(y_buf.at[j, give, :], y_ref.at[:, y_cols(other_col, j)], y_send.at[j], y_recv.at[j], to_col)

    def pass_on(j):
        slot = wo_slot(across, j)
        remote(slot, slot, wo_send.at[1, j], wo_recv.at[1, j], to_across).wait_recv()
        wo_pass(j).start()

    pass_on(0)
    for h in range(heads):
        other_half(h).wait_recv()

    def finish(j, carry):
        @pl.when(j + 1 < chunks)
        def _():
            pass_on(j + 1)

        slot = wo_slot(mate, j)
        remote(slot, slot, wo_send.at[0, j], wo_recv.at[0, j], to_mate).wait_recv()
        slot = wo_slot(diagonal, j)
        remote(slot, slot, wo_send.at[2, j], wo_recv.at[2, j], to_mate).wait_recv()
        total = jnp.zeros((rows, width), jnp.float32)
        for c in range(TP):
            for s in range(SP):
                k = (c * SP + s) * heads * HEAD_DIM
                total += jnp.dot(
                    o_all[c, s], wo_all[k:k + heads * HEAD_DIM, wo_cols(j)],
                    preferred_element_type=jnp.float32,
                )
        y_buf[j] = total.astype(jnp.bfloat16)
        y_copy(j).start()
        y_local(j).start()
        return carry

    lax.fori_loop(0, chunks, finish, 0)

    for j in range(chunks):
        y_arrive(j).wait_recv()
        y_local(j).wait()
        y_copy(j).wait_send()
        wo_to_across(j).wait_send()
        wo_to_mate(j).wait_send()
        wo_pass(j).wait_send()
    for copy in x_sends + doc_sends:
        copy.wait_send()
    for h in range(heads):
        for i in range(3):
            w_copy(i, h).wait_send()
            o_copy(i, h).wait_send()
        o_pass(h).wait_send()


def solution(mesh):
    def device_block(x_block, doc_block, wqkv_block, wout_block):
        rows, half = x_block.shape
        depth = wqkv_block.shape[0]
        heads = wqkv_block.shape[1] // (TRIPLE * SP)
        cols = wout_block.shape[1]
        chunks = 8
        width = cols // chunks
        bf16 = jnp.bfloat16
        dma = pltpu.SemaphoreType.DMA
        return pl.pallas_call(
            block_kernel,
            out_shape=jax.ShapeDtypeStruct((rows // TP, cols * TP), bf16),
            in_specs=[pl.BlockSpec(memory_space=pl.ANY)] * 4,
            out_specs=pl.BlockSpec(memory_space=pl.ANY),
            scratch_shapes=[
                pltpu.VMEM((TP, SP * rows, half), bf16),
                pltpu.VMEM((heads, SP * depth, TRIPLE), bf16),
                pltpu.VMEM((SP * depth, cols), bf16),
                pltpu.VMEM((TP, SP, rows, heads * HEAD_DIM), bf16),
                pltpu.VMEM((heads, SP * rows, HEAD_DIM), bf16),
                pltpu.VMEM((SP * rows, TRIPLE), bf16),
                pltpu.VMEM((chunks, rows, width), bf16),
                pltpu.VMEM((SP, 1, rows), jnp.int32),
                pltpu.VMEM((SP * rows, HEAD_DIM), jnp.int32),
                dma((2,)),
                dma((heads,)),
                dma((7,)),
                dma((7,)),
                dma((3,)),
                dma((3,)),
                dma((heads, 3)),
                dma((heads, 3)),
                dma,
                dma((3, chunks)),
                dma((3, chunks)),
                dma((heads, 3)),
                dma((heads, 3)),
                dma((heads,)),
                dma((heads,)),
                dma((chunks,)),
                dma((chunks,)),
                dma((chunks,)),
            ],
            compiler_params=pltpu.CompilerParams(
                collective_id=0, has_side_effects=True, vmem_limit_bytes=66 * 1024 * 1024 - 2 * 1024 * 1024 - 65536,
            ),
            name="attention_block",
        )(x_block, doc_block.reshape(1, rows), wqkv_block, wout_block)

    return jax.shard_map(
        device_block,
        mesh=mesh,
        in_specs=(P(("dp", "sp"), "tp"), P(("dp", "sp")), P("sp", "tp"), P("sp", "tp")),
        out_specs=P(("dp", "sp", "tp"), None),
        check_vma=False,
    )
```

```python
import functools

import jax
import jax.numpy as jnp
from jax import lax
from jax.experimental import pallas as pl
from jax.experimental.pallas import tpu as pltpu
from jax.sharding import PartitionSpec as P

HEAD_DIM = 128
SOFTMAX_SCALE = HEAD_DIM ** -0.5
TRIPLE = 3 * HEAD_DIM
SP = 4
TP = 2
WIDTHS = (384, 384, 384, 384, 256, 128, 128)
EARLY = 2


def block_kernel(
    x_ref, doc_ref, wqkv_ref, wout_ref, y_ref,
    x_all, w_all, wo_all, o_all, qkv, doc_all,
    local_sem, w_local_sem, x_send, x_recv, doc_send, doc_recv, w_send, w_recv,
    wo_local_sem, wo_send, wo_recv, o_send, o_recv, of_send, of_recv, y_send, y_recv,
):
    me = lax.axis_index("sp")
    col = lax.axis_index("tp")
    rows, half = x_ref.shape
    depth = wqkv_ref.shape[0]
    heads = w_all.shape[0]
    chunks = len(WIDTHS)
    starts = [sum(WIDTHS[:j]) for j in range(chunks)]
    cols = wout_ref.shape[1]
    other_col = 1 - col
    chip = me // 2
    core = lax.rem(me, 2)
    mate = chip * 2 + 1 - core
    across = (1 - chip) * 2 + core
    diagonal = (1 - chip) * 2 + 1 - core
    peers = (mate, across, diagonal)

    barrier = pltpu.get_barrier_semaphore()
    for peer in peers:
        pl.semaphore_signal(barrier, inc=1, device_id={"sp": peer}, device_id_type=pl.DeviceIdType.MESH)
    pl.semaphore_signal(barrier, inc=1, device_id={"tp": other_col}, device_id_type=pl.DeviceIdType.MESH)
    pl.semaphore_wait(barrier, 4)

    def remote(src, dst, send, recv, where):
        return pltpu.make_async_remote_copy(
            src_ref=src, dst_ref=dst, send_sem=send, recv_sem=recv,
            device_id=where, device_id_type=pl.DeviceIdType.MESH,
        )

    def x_slot(c, s):
        return x_all.at[c, pl.ds(pl.multiple_of(s * rows, rows), rows), :]

    def x_copy(i, c, s, where, src=None):
        slot = x_slot(c, s)
        return remote(slot if src is None else src, slot, x_send.at[i], x_recv.at[i], where)

    to_mate, to_across, to_col = {"sp": mate}, {"sp": across}, {"tp": other_col}

    x_sends = [
        x_copy(0, col, me, to_mate, x_ref),
        x_copy(1, col, me, to_across, x_ref),
        x_copy(2, col, me, to_col, x_ref),
    ]
    for copy in x_sends:
        copy.start()
    x_local = pltpu.make_async_copy(x_ref, x_slot(col, me), local_sem.at[0])
    x_local.start()
    doc_local = pltpu.make_async_copy(doc_ref, doc_all.at[me], local_sem.at[1])
    doc_local.start()
    doc_sends = []
    for i, peer in enumerate(peers):
        copy = remote(doc_ref, doc_all.at[me], doc_send.at[i], doc_recv.at[i], {"sp": peer})
        copy.start()
        doc_sends.append(copy)

    def w_cols(owner, h):
        start = pl.multiple_of((owner * heads + h) * TRIPLE, TRIPLE)
        return wqkv_ref.at[:, pl.ds(start, TRIPLE)]

    def w_slot(h, s):
        return w_all.at[h, pl.ds(pl.multiple_of(s * depth, depth), depth), :]

    def w_copy(i, h):
        return remote(w_cols(peers[i], h), w_slot(h, me), w_send.at[h, i], w_recv.at[h, i], {"sp": peers[i]})

    def w_local(h):
        return pltpu.make_async_copy(w_cols(me, h), w_slot(h, me), w_local_sem.at[h])

    for h in range(heads):
        w_copy(1, h).start()
        w_copy(2, h).start()
        w_copy(0, h).start()
        w_local(h).start()

    def wo_cols(j):
        return pl.ds(starts[j], WIDTHS[j])

    def wo_slot(s, j):
        return wo_all.at[pl.ds(pl.multiple_of(s * depth, depth), depth), wo_cols(j)]

    wo_local = pltpu.make_async_copy(wout_ref, wo_all.at[pl.ds(pl.multiple_of(me * depth, depth), depth), :], wo_local_sem)
    wo_local.start()

    x_copy(2, other_col, me, to_col).wait_recv()
    x_sends.append(x_copy(5, other_col, me, to_mate))
    x_sends[-1].start()
    x_copy(1, col, across, to_across).wait_recv()
    x_sends.append(x_copy(4, col, across, to_col))
    x_sends[-1].start()
    x_sends.append(x_copy(3, col, across, to_mate))
    x_sends[-1].start()

    doc_local.wait()
    for i, peer in enumerate(peers):
        remote(doc_ref, doc_all.at[peer], doc_send.at[i], doc_recv.at[i], {"sp": peer}).wait_recv()

    x_copy(4, other_col, across, to_col).wait_recv()
    x_sends.append(x_copy(6, other_col, across, to_mate))
    x_sends[-1].start()
    x_local.wait()
    x_copy(0, col, mate, to_mate).wait_recv()
    x_copy(3, col, diagonal, to_mate).wait_recv()
    x_copy(5, other_col, mate, to_mate).wait_recv()
    x_copy(6, other_col, diagonal, to_mate).wait_recv()

    def wo_to_mate(j):
        return remote(wout_ref.at[:, wo_cols(j)], wo_slot(me, j), wo_send.at[0, j], wo_recv.at[0, j], to_mate)

    def wo_to_across(j):
        return remote(wout_ref.at[:, wo_cols(j)], wo_slot(me, j), wo_send.at[1, j], wo_recv.at[1, j], to_across)

    def wo_pass(j):
        slot = wo_slot(across, j)
        return remote(slot, slot, wo_send.at[2, j], wo_recv.at[2, j], to_mate)

    def o_slot(c, s, h):
        return o_all.at[c, s, :, pl.ds(pl.multiple_of(h * HEAD_DIM, HEAD_DIM), HEAD_DIM)]

    def o_copy(i, h):
        src = w_all.at[h, pl.ds(pl.multiple_of(peers[i] * rows, rows), rows), pl.ds(0, HEAD_DIM)]
        return remote(src, o_slot(col, me, h), o_send.at[h, i], o_recv.at[h, i], {"sp": peers[i]})

    def o_pass(h):
        slot = o_all.at[col, :, :, pl.ds(pl.multiple_of(h * HEAD_DIM, HEAD_DIM), HEAD_DIM)]
        return remote(slot, slot, of_send.at[h], of_recv.at[h], to_col)

    def o_collect(h):
        for i in range(3):
            remote(o_slot(col, peers[i], h), o_slot(col, peers[i], h), o_send.at[h, i], o_recv.at[h, i], {"sp": peers[i]}).wait_recv()
        o_pass(h).start()

    early = EARLY

    def one_head(h, carry):
        w_local(h).wait()
        for i in range(3):
            remote(w_cols(peers[i], h), w_slot(h, peers[i]), w_send.at[h, i], w_recv.at[h, i], {"sp": peers[i]}).wait_recv()

        @pl.when(h == heads - 2)
        def _():
            for j in range(early):
                wo_to_across(j).start()

        def project(r, carry):
            tile = pl.ds(pl.multiple_of(r * rows, rows), rows)
            total = jnp.dot(x_all[0, tile, :], w_all[h, :half, :], preferred_element_type=jnp.float32)
            total += jnp.dot(x_all[1, tile, :], w_all[h, half:, :], preferred_element_type=jnp.float32)
            qkv[tile, :] = total.astype(jnp.bfloat16)
            return carry

        lax.fori_loop(0, SP, project, 0)

        docs = jnp.concatenate([doc_all[s] for s in range(SP)], axis=1)

        def attend(r, carry):
            tile = pl.ds(pl.multiple_of(r * 256, 256), 256)
            query = qkv[tile, :HEAD_DIM]
            scores = lax.dot_general(
                query, qkv[:, HEAD_DIM:2 * HEAD_DIM], (((1,), (1,)), ((), ())),
                preferred_element_type=jnp.float32,
            ) * SOFTMAX_SCALE
            own = doc_all[r // 2, :, pl.ds(pl.multiple_of(lax.rem(r, 2) * 256, 256), 256)]
            same = jnp.broadcast_to(own, (HEAD_DIM, 256)).T[:, :1] == docs
            scores = jnp.where(same, scores, -jnp.inf)
            top = jnp.max(scores, axis=1, keepdims=True)
            weights = jnp.exp(scores - top)
            weights = weights * (1.0 / jnp.sum(weights, axis=1, keepdims=True))
            out = jnp.dot(weights.astype(jnp.bfloat16), qkv[:, 2 * HEAD_DIM:], preferred_element_type=jnp.float32)
            w_all[h, tile, :HEAD_DIM] = out.astype(jnp.bfloat16)
            return carry

        lax.fori_loop(0, SP * rows // 256, attend, 0)
        mine = pl.ds(pl.multiple_of(me * rows, rows), rows)
        o_all[col, me, :, pl.ds(pl.multiple_of(h * HEAD_DIM, HEAD_DIM), HEAD_DIM)] = w_all[h, mine, :HEAD_DIM]
        for i in (1, 2, 0):
            o_copy(i, h).start()

        @pl.when(h >= 1)
        def _():
            o_collect(h - 1)

        return carry

    lax.fori_loop(0, heads, one_head, 0)
    for j in range(early, chunks):
        wo_to_across(j).start()
    for j in range(chunks):
        wo_to_mate(j).start()
    wo_local.wait()
    o_collect(heads - 1)

    def other_half(h):
        slot = o_all.at[other_col, :, :, pl.ds(pl.multiple_of(h * HEAD_DIM, HEAD_DIM), HEAD_DIM)]
        return remote(slot, slot, of_send.at[h], of_recv.at[h], to_col)

    span = rows // 2
    keep = pl.ds(pl.multiple_of(col * span, span), span)
    give = pl.ds(pl.multiple_of(other_col * span, span), span)

    def y_cols(c, j):
        return pl.ds(pl.multiple_of(c * cols + starts[j], HEAD_DIM), WIDTHS[j])

    def given_slot(j):
        return w_all.at[heads - 1, pl.ds(SP * rows + j * span, span), pl.ds(0, WIDTHS[j])]

    def y_copy(j):
        return remote(given_slot(j), y_ref.at[:, y_cols(col, j)], y_send.at[j], y_recv.at[j], to_col)

    def y_arrive(j):
        return remote(given_slot(j), y_ref.at[:, y_cols(other_col, j)], y_send.at[j], y_recv.at[j], to_col)

    def part(owner, piece, j):
        total = None
        for i in range(2):
            block = (owner % 2) * 2 + i
            first = pl.multiple_of(owner * depth + i * (depth // 2), depth // 2)
            term = jnp.dot(
                o_all[owner // 2, block, piece, :], wo_all[pl.ds(first, depth // 2), wo_cols(j)],
                preferred_element_type=jnp.float32,
            )
            total = term if total is None else total + term
        return total

    for h in range(heads):
        other_half(h).wait_recv()

    for j in range(chunks):
        slot = wo_slot(mate, j)
        remote(slot, slot, wo_send.at[0, j], wo_recv.at[0, j], to_mate).wait_recv()
        given = part(me, give, j) + part(mate, give, j)
        kept = part(me, keep, j) + part(mate, keep, j)
        slot = wo_slot(across, j)
        remote(slot, slot, wo_send.at[1, j], wo_recv.at[1, j], to_across).wait_recv()
        wo_pass(j).start()
        given += part(across, give, j)
        kept += part(across, keep, j)
        slot = wo_slot(diagonal, j)
        remote(slot, slot, wo_send.at[2, j], wo_recv.at[2, j], to_mate).wait_recv()
        given += part(diagonal, give, j)
        w_all[heads - 1, pl.ds(SP * rows + j * span, span), :WIDTHS[j]] = given.astype(jnp.bfloat16)
        kept += part(diagonal, keep, j)
        y_copy(j).start()
        y_ref[:, y_cols(col, j)] = kept.astype(jnp.bfloat16)

    for j in range(chunks):
        y_arrive(j).wait_recv()
        y_copy(j).wait_send()
        wo_to_across(j).wait_send()
        wo_to_mate(j).wait_send()
        wo_pass(j).wait_send()
    for copy in x_sends + doc_sends:
        copy.wait_send()
    for h in range(heads):
        for i in range(3):
            w_copy(i, h).wait_send()
            o_copy(i, h).wait_send()
        o_pass(h).wait_send()


def solution(mesh):
    def device_block(x_block, doc_block, wqkv_block, wout_block):
        rows, half = x_block.shape
        depth = wqkv_block.shape[0]
        heads = wqkv_block.shape[1] // (TRIPLE * SP)
        cols = wout_block.shape[1]
        chunks = len(WIDTHS)
        bf16 = jnp.bfloat16
        dma = pltpu.SemaphoreType.DMA
        return pl.pallas_call(
            block_kernel,
            out_shape=pltpu.VMEM((rows // TP, cols * TP), bf16),
            in_specs=[pl.BlockSpec(memory_space=pl.ANY)] * 4,
            out_specs=pl.BlockSpec(memory_space=pltpu.VMEM),
            scratch_shapes=[
                pltpu.VMEM((TP, SP * rows, half), bf16),
                pltpu.VMEM((heads, SP * depth, TRIPLE), bf16),
                pltpu.VMEM((SP * depth, cols), bf16),
                pltpu.VMEM((TP, SP, rows, heads * HEAD_DIM), bf16),
                pltpu.VMEM((SP * rows, TRIPLE), bf16),
                pltpu.VMEM((SP, 1, rows), jnp.int32),
                dma((2,)),
                dma((heads,)),
                dma((7,)),
                dma((7,)),
                dma((3,)),
                dma((3,)),
                dma((heads, 3)),
                dma((heads, 3)),
                dma,
                dma((3, chunks)),
                dma((3, chunks)),
                dma((heads, 3)),
                dma((heads, 3)),
                dma((heads,)),
                dma((heads,)),
                dma((chunks,)),
                dma((chunks,)),
            ],
            compiler_params=pltpu.CompilerParams(
                collective_id=0, has_side_effects=True, vmem_limit_bytes=57 * 1024 * 1024,
            ),
            name="attention_block",
        )(x_block, doc_block.reshape(1, rows), wqkv_block, wout_block)

    return jax.shard_map(
        device_block,
        mesh=mesh,
        in_specs=(P(("dp", "sp"), "tp"), P(("dp", "sp")), P("sp", "tp"), P("sp", "tp")),
        out_specs=P(("dp", "sp", "tp"), None),
        check_vma=False,
    )
```

```python
import jax
import jax.numpy as jnp
from jax import lax
from jax.experimental import pallas as pl
from jax.experimental.pallas import tpu as pltpu
from jax.sharding import PartitionSpec as P

HEAD_DIM = 128
SOFTMAX_SCALE = HEAD_DIM ** -0.5
TRIPLE = 3 * HEAD_DIM
SP = 4
TP = 2
WIDTH = 128
EARLY = 4
QUERIES = 256


def block_kernel(
    x_ref, doc_ref, wqkv_ref, wout_ref, y_ref,
    x_all, w_all, wo_all, o_all, qkv, doc_all,
    local_sem, x_send, x_recv, doc_send, doc_recv, w_send, w_recv, wo_send, wo_mate_recv,
    wo_recv, wo_pass_recv, o_send, o_recv, of_send, of_recv, y_send, y_recv,
):
    me = lax.axis_index("sp")
    col = lax.axis_index("tp")
    rows, half = x_ref.shape
    depth = wqkv_ref.shape[0]
    heads = w_all.shape[0]
    cols = wout_ref.shape[1]
    chunks = cols // WIDTH
    other_col = 1 - col
    chip = me // 2
    core = lax.rem(me, 2)
    mate = chip * 2 + 1 - core
    across = (1 - chip) * 2 + core
    diagonal = (1 - chip) * 2 + 1 - core
    peers = (mate, across, diagonal)
    to_mate, to_across, to_diagonal, to_col = {"sp": mate}, {"sp": across}, {"sp": diagonal}, {"tp": other_col}
    to_peers = (to_mate, to_across, to_diagonal)

    barrier = pltpu.get_barrier_semaphore()
    for where in (to_across, to_diagonal, to_col, to_mate):
        pl.semaphore_signal(barrier, inc=1, device_id=where, device_id_type=pl.DeviceIdType.MESH)
    pl.semaphore_wait(barrier, 4)

    def remote(src, dst, send, recv, where):
        return pltpu.make_async_remote_copy(
            src_ref=src, dst_ref=dst, send_sem=send, recv_sem=recv,
            device_id=where, device_id_type=pl.DeviceIdType.MESH,
        )

    def take(sem, ref):
        remote(ref, ref, sem, sem, to_mate).wait_recv()

    def local(src, dst, i):
        return pltpu.make_async_copy(src, dst, local_sem.at[i])

    def at(i, size):
        return pl.ds(pl.multiple_of(i * size, size), size)

    def x_slot(c, s):
        return x_all.at[c, at(s, rows), :]

    def x_pass(c, s, send, recv, where):
        remote(x_slot(c, s), x_slot(c, s), x_send.at[send], x_recv.at[recv], where).start()

    own_x = x_slot(col, me)
    remote(x_ref, own_x, x_send.at[0], x_recv.at[0], to_across).start()
    remote(x_ref, own_x, x_send.at[0], x_recv.at[1], to_col).start()
    remote(x_ref, own_x, x_send.at[0], x_recv.at[3], to_mate).start()
    local(x_ref, own_x, 0).start()
    for where in to_peers:
        remote(doc_ref, doc_all.at[me], doc_send, doc_recv, where).start()
    local(doc_ref, doc_all.at[me], 1).start()

    def w_cols(owner, h):
        return wqkv_ref.at[:, at(owner * heads + h, TRIPLE)]

    def w_slot(h, s):
        return w_all.at[h, at(s, depth), :]

    def w_go(i, h):
        remote(w_cols(peers[i], h), w_slot(h, me), w_send, w_recv.at[h], to_peers[i]).start()

    for h in range(heads):
        if h < heads - 1:
            w_go(1, h)
            w_go(2, h)
        w_go(0, h)
        local(w_cols(me, h), w_slot(h, me), 2).start()
    own_wo = wo_all.at[at(me, depth), :]
    local(wout_ref, own_wo, 3).start()

    take(x_recv.at[1], x_slot(other_col, me))
    x_pass(other_col, me, 1, 3, to_mate)
    take(x_recv.at[0], x_slot(col, across))
    x_pass(col, across, 1, 2, to_col)
    x_pass(col, across, 1, 3, to_mate)
    take(x_recv.at[2], x_slot(other_col, across))
    x_pass(other_col, across, 1, 3, to_mate)
    local(x_ref, own_x, 0).wait()
    local(doc_ref, doc_all.at[me], 1).wait()
    local(w_all.at[0], w_all.at[0], 2).wait()
    local(wout_ref, own_wo, 3).wait()
    take(doc_recv, doc_all.at[pl.ds(0, SP - 1)])
    take(x_recv.at[3], x_all.at[0])

    def wo_slot(s, j):
        return wo_all.at[at(s, depth), at(j, WIDTH)]

    def wo_go(j):
        remote(wout_ref.at[:, at(j, WIDTH)], wo_slot(me, j), wo_send.at[1], wo_recv.at[j], to_across).start()

    def wo_pass(j):
        remote(wo_slot(across, j), wo_slot(across, j), wo_send.at[2], wo_pass_recv.at[j], to_mate).start()

    def o_go(i, h):
        src = w_all.at[h, at(peers[i], rows), pl.ds(0, HEAD_DIM)]
        dst = o_all.at[col, me, :, at(h, HEAD_DIM)]
        remote(src, dst, o_send, o_recv.at[h], to_peers[i]).start()

    def o_pass(h):
        take(o_recv.at[h], w_all.at[0, pl.ds(0, rows), :])
        slot = o_all.at[col, :, :, at(h, HEAD_DIM)]
        remote(slot, slot, of_send, of_recv, to_col).start()

    def one_head(h, carry):
        take(w_recv.at[h], w_all.at[0, pl.ds(0, (SP - 1) * depth), :])

        def project(r, carry):
            tile = at(r, rows)
            total = jnp.dot(x_all[0, tile, :], w_all[h, :half, :], preferred_element_type=jnp.float32)
            total += jnp.dot(x_all[1, tile, :], w_all[h, half:, :], preferred_element_type=jnp.float32)
            qkv[tile, :] = total.astype(jnp.bfloat16)
            return carry

        lax.fori_loop(0, SP, project, 0)

        docs = jnp.concatenate([doc_all[s] for s in range(SP)], axis=1)
        per_block = rows // QUERIES

        def attend(r, carry):
            tile = at(r, QUERIES)
            scores = lax.dot_general(
                qkv[tile, :HEAD_DIM], qkv[:, HEAD_DIM:2 * HEAD_DIM], (((1,), (1,)), ((), ())),
                preferred_element_type=jnp.float32,
            ) * SOFTMAX_SCALE
            own = doc_all[r // per_block, :, at(lax.rem(r, per_block), QUERIES)]
            same = jnp.broadcast_to(own, (HEAD_DIM, QUERIES)).T[:, :1] == docs
            scores = jnp.where(same, scores, -jnp.inf)
            top = jnp.max(scores, axis=1, keepdims=True)
            weights = jnp.exp(scores - top)
            weights = weights * (1.0 / jnp.sum(weights, axis=1, keepdims=True))
            out = jnp.dot(weights.astype(jnp.bfloat16), qkv[:, 2 * HEAD_DIM:], preferred_element_type=jnp.float32)
            w_all[h, tile, :HEAD_DIM] = out.astype(jnp.bfloat16)
            return carry

        lax.fori_loop(0, SP * per_block, attend, 0)
        o_all[col, me, :, at(h, HEAD_DIM)] = w_all[h, at(me, rows), :HEAD_DIM]
        for i in (1, 2, 0):
            o_go(i, h)

        @pl.when(h == 0)
        def _():
            w_go(1, heads - 1)
            w_go(2, heads - 1)
            remote(wout_ref, own_wo, wo_send.at[0], wo_mate_recv, to_mate).start()

        @pl.when(h == heads - 2)
        def _():
            for j in range(EARLY):
                wo_go(j)
            o_pass(0)

        return carry

    lax.fori_loop(0, heads, one_head, 0)
    for j in range(EARLY, chunks):
        wo_go(j)
    for h in range(1, heads):
        o_pass(h)

    span = rows // 2
    keep = at(col, span)
    give = at(other_col, span)

    def y_go(j):
        src = w_all.at[heads - 1, at(j, span), pl.ds(HEAD_DIM, WIDTH)]
        remote(src, y_ref.at[:, at(col * chunks + j, WIDTH)], y_send, y_recv, to_col).start()

    def part(owner, piece, j):
        total = None
        for i in range(2):
            term = jnp.dot(
                o_all[owner // 2, lax.rem(owner, 2) * 2 + i, piece, :], wo_all[at(owner * 2 + i, depth // 2), at(j, WIDTH)],
                preferred_element_type=jnp.float32,
            )
            total = term if total is None else total + term
        return total

    take(wo_mate_recv, wo_all.at[pl.ds(0, depth), :])
    take(of_recv, o_all.at[0])

    take(x_send.at[0], x_all.at[0, pl.ds(0, 3 * rows), :])
    take(x_send.at[1], x_all.at[0])
    take(doc_send, doc_all.at[pl.ds(0, SP - 1)])
    take(w_send, w_all.at[pl.ds(0, SP - 1)])
    take(o_send, o_all.at[0, pl.ds(0, SP - 1)])
    take(of_send, o_all.at[0])
    take(wo_send.at[0], wo_all.at[pl.ds(0, depth), :])

    def finish(j, carry):
        given = part(me, give, j) + part(mate, give, j)
        kept = part(me, keep, j) + part(mate, keep, j)
        take(wo_recv.at[j], wo_slot(across, j))
        wo_pass(j)
        given += part(across, give, j)
        kept += part(across, keep, j)
        take(wo_pass_recv.at[j], wo_slot(diagonal, j))
        given += part(diagonal, give, j)
        w_all[heads - 1, at(j, span), HEAD_DIM:HEAD_DIM + WIDTH] = given.astype(jnp.bfloat16)
        y_go(j)
        kept += part(diagonal, keep, j)
        y_ref[:, at(col * chunks + j, WIDTH)] = kept.astype(jnp.bfloat16)
        return carry

    lax.fori_loop(0, chunks, finish, 0)
    take(wo_send.at[1], wo_all.at[pl.ds(0, depth), :])
    take(wo_send.at[2], wo_all.at[pl.ds(0, depth), :])
    take(y_send, y_ref.at[:, pl.ds(0, cols)])
    take(y_recv, y_ref.at[:, pl.ds(0, cols)])


def solution(mesh):
    def device_block(x_block, doc_block, wqkv_block, wout_block):
        rows, half = x_block.shape
        depth = wqkv_block.shape[0]
        heads = wqkv_block.shape[1] // (TRIPLE * SP)
        cols = wout_block.shape[1]
        chunks = cols // WIDTH
        bf16 = jnp.bfloat16
        dma = pltpu.SemaphoreType.DMA
        return pl.pallas_call(
            block_kernel,
            out_shape=pltpu.VMEM((rows // TP, cols * TP), bf16),
            in_specs=[pl.BlockSpec(memory_space=pl.ANY)] * 4,
            out_specs=pl.BlockSpec(memory_space=pltpu.VMEM),
            scratch_shapes=[
                pltpu.VMEM((TP, SP * rows, half), bf16),
                pltpu.VMEM((heads, SP * depth, TRIPLE), bf16),
                pltpu.VMEM((SP * depth, cols), bf16),
                pltpu.VMEM((TP, SP, rows, heads * HEAD_DIM), bf16),
                pltpu.VMEM((SP * rows, TRIPLE), bf16),
                pltpu.VMEM((SP, 1, rows), jnp.int32),
                dma((4,)),
                dma((2,)),
                dma((4,)),
                dma,
                dma,
                dma,
                dma((heads,)),
                dma((3,)),
                dma,
                dma((chunks,)),
                dma((chunks,)),
                dma,
                dma((heads,)),
                dma,
                dma,
                dma,
                dma,
            ],
            compiler_params=pltpu.CompilerParams(
                collective_id=0, has_side_effects=True, vmem_limit_bytes=57 * 1024 * 1024,
            ),
            name="attention_block",
        )(x_block, doc_block.reshape(1, rows), wqkv_block, wout_block)

    return jax.shard_map(
        device_block,
        mesh=mesh,
        in_specs=(P(("dp", "sp"), "tp"), P(("dp", "sp")), P("sp", "tp"), P("sp", "tp")),
        out_specs=P(("dp", "sp", "tp"), None),
        check_vma=False,
    )
```

```python
import jax
import jax.numpy as jnp
from jax import lax
from jax.experimental import pallas as pl
from jax.experimental.pallas import tpu as pltpu
from jax.sharding import PartitionSpec as P

HEAD_DIM = 128
SOFTMAX_SCALE = HEAD_DIM ** -0.5
TRIPLE = 3 * HEAD_DIM
SP = 4
TP = 2
WIDTH = 128
EARLY = 4
QUERIES = 256


def block_kernel(
    x_ref, doc_ref, wqkv_ref, wout_ref, y_ref,
    x_all, w_all, wo_all, o_all, o_mate, early_sums, qkv, doc_all,
    local_sem, x_send, x_recv, doc_send, doc_recv, w_send, w_recv, wo_send, wo_mate_recv,
    wo_recv, wo_pass_recv, o_send, o_recv, of_send, of_recv, y_send, y_recv,
    last_send, last_recv, mate_send, mate_recv,
):
    me = lax.axis_index("sp")
    col = lax.axis_index("tp")
    rows, half = x_ref.shape
    depth = wqkv_ref.shape[0]
    heads = w_all.shape[0]
    cols = wout_ref.shape[1]
    chunks = cols // WIDTH
    last = chunks - 1
    other_col = 1 - col
    chip = me // 2
    core = lax.rem(me, 2)
    mate = chip * 2 + 1 - core
    across = (1 - chip) * 2 + core
    diagonal = (1 - chip) * 2 + 1 - core
    peers = (mate, across, diagonal)
    to_mate, to_across, to_diagonal, to_col = {"sp": mate}, {"sp": across}, {"sp": diagonal}, {"tp": other_col}
    to_peers = (to_mate, to_across, to_diagonal)
    to_col_mate = {"sp": mate, "tp": other_col}

    barrier = pltpu.get_barrier_semaphore()
    for where in (to_across, to_diagonal, to_col, to_col_mate, to_mate):
        pl.semaphore_signal(barrier, inc=1, device_id=where, device_id_type=pl.DeviceIdType.MESH)
    pl.semaphore_wait(barrier, 5)

    def remote(src, dst, send, recv, where):
        return pltpu.make_async_remote_copy(
            src_ref=src, dst_ref=dst, send_sem=send, recv_sem=recv,
            device_id=where, device_id_type=pl.DeviceIdType.MESH,
        )

    def take(sem, ref):
        remote(ref, ref, sem, sem, to_mate).wait_recv()

    def local(src, dst, i):
        return pltpu.make_async_copy(src, dst, local_sem.at[i])

    def at(i, size):
        return pl.ds(pl.multiple_of(i * size, size), size)

    def x_slot(c, s):
        return x_all.at[c, at(s, rows), :]

    def x_pass(c, s, send, recv, where):
        remote(x_slot(c, s), x_slot(c, s), x_send.at[send], x_recv.at[recv], where).start()

    own_x = x_slot(col, me)
    remote(x_ref, own_x, x_send.at[0], x_recv.at[0], to_across).start()
    remote(x_ref, own_x, x_send.at[0], x_recv.at[1], to_col).start()
    remote(x_ref, own_x, x_send.at[0], x_recv.at[3], to_mate).start()
    local(x_ref, own_x, 0).start()
    for where in to_peers:
        remote(doc_ref, doc_all.at[me], doc_send, doc_recv, where).start()
    local(doc_ref, doc_all.at[me], 1).start()

    def w_cols(owner, h):
        return wqkv_ref.at[:, at(owner * heads + h, TRIPLE)]

    def w_slot(h, s):
        return w_all.at[h, at(s, depth), :]

    def w_go(i, h):
        remote(w_cols(peers[i], h), w_slot(h, me), w_send, w_recv.at[h], to_peers[i]).start()

    for h in range(heads):
        if h < heads - 1:
            w_go(1, h)
            w_go(2, h)
        w_go(0, h)
        local(w_cols(me, h), w_slot(h, me), 2).start()
    own_wo = wo_all.at[at(me, depth), :]
    local(wout_ref, own_wo, 3).start()

    take(x_recv.at[1], x_slot(other_col, me))
    x_pass(other_col, me, 1, 3, to_mate)
    take(x_recv.at[0], x_slot(col, across))
    x_pass(col, across, 1, 2, to_col)
    x_pass(col, across, 1, 3, to_mate)
    take(x_recv.at[2], x_slot(other_col, across))
    x_pass(other_col, across, 1, 3, to_mate)
    local(x_ref, own_x, 0).wait()
    local(doc_ref, doc_all.at[me], 1).wait()
    local(w_all.at[0], w_all.at[0], 2).wait()
    local(wout_ref, own_wo, 3).wait()
    take(doc_recv, doc_all.at[pl.ds(0, SP - 1)])
    take(x_recv.at[3], x_all.at[0])

    def wo_slot(s, j):
        return wo_all.at[at(s, depth), at(j, WIDTH)]

    def wo_go(j):
        remote(wout_ref.at[:, at(j, WIDTH)], wo_slot(me, j), wo_send.at[1], wo_recv.at[j], to_across).start()

    def wo_pass(j):
        remote(wo_slot(across, j), wo_slot(across, j), wo_send.at[2], wo_pass_recv.at[j], to_mate).start()

    def o_go(i, h):
        src = w_all.at[h, at(peers[i], rows), pl.ds(0, HEAD_DIM)]
        dst = o_all.at[col, me, :, at(h, HEAD_DIM)]
        remote(src, dst, o_send, o_recv.at[h], to_peers[i]).start()

    def o_pass(h):
        take(o_recv.at[h], w_all.at[0, pl.ds(0, rows), :])
        slot = o_all.at[col, :, :, at(h, HEAD_DIM)]
        remote(slot, slot, of_send, of_recv, to_col).start()

    def one_head(h, carry):
        take(w_recv.at[h], w_all.at[0, pl.ds(0, (SP - 1) * depth), :])

        def project(r, carry):
            tile = at(r, rows)
            total = jnp.dot(x_all[0, tile, :], w_all[h, :half, :], preferred_element_type=jnp.float32)
            total += jnp.dot(x_all[1, tile, :], w_all[h, half:, :], preferred_element_type=jnp.float32)
            qkv[tile, :] = total.astype(jnp.bfloat16)
            return carry

        lax.fori_loop(0, SP, project, 0)

        docs = jnp.concatenate([doc_all[s] for s in range(SP)], axis=1)
        per_block = rows // QUERIES

        def attend(r, carry):
            tile = at(r, QUERIES)
            scores = lax.dot_general(
                qkv[tile, :HEAD_DIM], qkv[:, HEAD_DIM:2 * HEAD_DIM], (((1,), (1,)), ((), ())),
                preferred_element_type=jnp.float32,
            ) * SOFTMAX_SCALE
            own = doc_all[r // per_block, :, at(lax.rem(r, per_block), QUERIES)]
            same = jnp.broadcast_to(own, (HEAD_DIM, QUERIES)).T[:, :1] == docs
            scores = jnp.where(same, scores, -jnp.inf)
            top = jnp.max(scores, axis=1, keepdims=True)
            weights = jnp.exp(scores - top)
            weights = weights * (1.0 / jnp.sum(weights, axis=1, keepdims=True))
            out = jnp.dot(weights.astype(jnp.bfloat16), qkv[:, 2 * HEAD_DIM:], preferred_element_type=jnp.float32)
            w_all[h, tile, :HEAD_DIM] = out.astype(jnp.bfloat16)
            return carry

        lax.fori_loop(0, SP * per_block, attend, 0)
        o_all[col, me, :, at(h, HEAD_DIM)] = w_all[h, at(me, rows), :HEAD_DIM]
        for i in (1, 2, 0):
            o_go(i, h)

        @pl.when(h == 0)
        def _():
            w_go(1, heads - 1)
            w_go(2, heads - 1)
            remote(wout_ref, own_wo, wo_send.at[0], wo_mate_recv, to_mate).start()

        @pl.when(h == heads - 2)
        def _():
            for j in range(EARLY):
                wo_go(j)
            o_pass(0)

        return carry

    lax.fori_loop(0, heads, one_head, 0)
    for j in range(EARLY, last):
        wo_go(j)
    take(wo_mate_recv, wo_all.at[pl.ds(0, depth), :])

    def last_go(i, src, owner):
        remote(src, wo_slot(owner, last), last_send, last_recv.at[i], to_across).start()

    @pl.when(core == 1)
    def _():
        last_go(0, wo_slot(mate, last), mate)
        last_go(1, wout_ref.at[:, at(last, WIDTH)], me)

    for h in range(1, heads):
        o_pass(h)

    span = rows // 2
    keep = at(col, span)
    give = at(other_col, span)

    def stage(j, k):
        return w_all.at[heads - 1, at(j, span), pl.ds(k * HEAD_DIM, WIDTH)]

    def y_slot(j):
        return y_ref.at[:, at(col * chunks + j, WIDTH)]

    def y_go(j):
        remote(stage(j, 1), y_slot(j), y_send, y_recv, to_col).start()

    def part(source, owner, piece, j):
        total = None
        for i in range(2):
            term = jnp.dot(
                source[owner // 2, lax.rem(owner, 2) * 2 + i, piece, :], wo_all[at(owner * 2 + i, depth // 2), at(j, WIDTH)],
                preferred_element_type=jnp.float32,
            )
            total = term if total is None else total + term
        return total

    take(of_recv, o_all.at[0])

    @pl.when(core == 0)
    def _():
        remote(o_all, o_mate, mate_send.at[0], mate_recv.at[0], to_mate).start()

    take(x_send.at[0], x_all.at[0, pl.ds(0, 3 * rows), :])
    take(x_send.at[1], x_all.at[0])
    take(doc_send, doc_all.at[pl.ds(0, SP - 1)])
    take(w_send, w_all.at[pl.ds(0, SP - 1)])
    take(o_send, o_all.at[0, pl.ds(0, SP - 1)])
    take(of_send, o_all.at[0])
    take(wo_send.at[0], wo_all.at[pl.ds(0, depth), :])

    blocks = ((o_mate, give), (o_all, give), (o_mate, keep), (o_all, keep))

    def finish(j, carry):
        @pl.when((j == last - 3) & (core == 1))
        def _():
            take(mate_recv.at[0], o_mate)
            for i, (source, piece) in enumerate(blocks):
                early_sums[i] = part(source, me, piece, last) + part(source, mate, piece, last)

        given = part(o_all, me, give, j) + part(o_all, mate, give, j)
        kept = part(o_all, me, keep, j) + part(o_all, mate, keep, j)
        take(wo_recv.at[j], wo_slot(across, j))
        wo_pass(j)
        given += part(o_all, across, give, j)
        kept += part(o_all, across, keep, j)
        take(wo_pass_recv.at[j], wo_slot(diagonal, j))
        given += part(o_all, diagonal, give, j)
        stage(j, 1)[...] = given.astype(jnp.bfloat16)
        y_go(j)
        kept += part(o_all, diagonal, keep, j)
        y_slot(j)[...] = kept.astype(jnp.bfloat16)
        return carry

    lax.fori_loop(0, last, finish, 0)
    most = pl.ds(0, last * WIDTH)

    @pl.when(core == 1)
    def _():
        take(last_recv.at[0], wo_slot(diagonal, last))
        totals = [early_sums[i] + part(source, diagonal, piece, last) for i, (source, piece) in enumerate(blocks)]
        take(last_recv.at[1], wo_slot(across, last))

        def whole(i):
            source, piece = blocks[i]
            return (totals[i] + part(source, across, piece, last)).astype(jnp.bfloat16)

        stage(0, 2)[...] = whole(0)
        to_col_mate_copy = remote(stage(0, 2), y_slot(last), mate_send.at[1], y_recv, to_col_mate)
        to_col_mate_copy.start()
        stage(last, 1)[...] = whole(1)
        y_go(last)
        stage(1, 2)[...] = whole(2)
        kept_copy = remote(stage(1, 2), y_slot(last), mate_send.at[2], mate_recv.at[1], to_mate)
        kept_copy.start()
        y_slot(last)[...] = whole(3)
        take(last_send, wo_all.at[pl.ds(0, depth), pl.ds(0, 2 * WIDTH)])
        take(y_send, y_ref.at[:, pl.ds(0, cols)])
        to_col_mate_copy.wait_send()
        kept_copy.wait_send()

    @pl.when(core == 0)
    def _():
        take(mate_send.at[0], o_all)
        take(y_send, y_ref.at[:, most])
        take(mate_recv.at[1], y_slot(last))

    take(wo_send.at[1], wo_all.at[pl.ds(0, depth), most])
    take(wo_send.at[2], wo_all.at[pl.ds(0, depth), most])
    take(y_recv, y_ref.at[:, pl.ds(0, cols)])


def solution(mesh):
    def device_block(x_block, doc_block, wqkv_block, wout_block):
        rows, half = x_block.shape
        depth = wqkv_block.shape[0]
        heads = wqkv_block.shape[1] // (TRIPLE * SP)
        cols = wout_block.shape[1]
        chunks = cols // WIDTH
        bf16 = jnp.bfloat16
        dma = pltpu.SemaphoreType.DMA
        return pl.pallas_call(
            block_kernel,
            out_shape=pltpu.VMEM((rows // TP, cols * TP), bf16),
            in_specs=[pl.BlockSpec(memory_space=pl.ANY)] * 4,
            out_specs=pl.BlockSpec(memory_space=pltpu.VMEM),
            scratch_shapes=[
                pltpu.VMEM((TP, SP * rows, half), bf16),
                pltpu.VMEM((heads, SP * depth, TRIPLE), bf16),
                pltpu.VMEM((SP * depth, cols), bf16),
                pltpu.VMEM((TP, SP, rows, heads * HEAD_DIM), bf16),
                pltpu.VMEM((TP, SP, rows, heads * HEAD_DIM), bf16),
                pltpu.VMEM((4, rows // 2, WIDTH), jnp.float32),
                pltpu.VMEM((SP * rows, TRIPLE), bf16),
                pltpu.VMEM((SP, 1, rows), jnp.int32),
                dma((4,)),
                dma((2,)),
                dma((4,)),
                dma,
                dma,
                dma,
                dma((heads,)),
                dma((3,)),
                dma,
                dma((chunks - 1,)),
                dma((chunks - 1,)),
                dma,
                dma((heads,)),
                dma,
                dma,
                dma,
                dma,
                dma,
                dma((2,)),
                dma((3,)),
                dma((2,)),
            ],
            compiler_params=pltpu.CompilerParams(
                collective_id=0, has_side_effects=True, vmem_limit_bytes=60 * 1024 * 1024,
            ),
            name="attention_block",
        )(x_block, doc_block.reshape(1, rows), wqkv_block, wout_block)

    return jax.shard_map(
        device_block,
        mesh=mesh,
        in_specs=(P(("dp", "sp"), "tp"), P(("dp", "sp")), P("sp", "tp"), P("sp", "tp")),
        out_specs=P(("dp", "sp", "tp"), None),
        check_vma=False,
    )
```

```python
import jax
import jax.numpy as jnp
from jax import lax
from jax.experimental import pallas as pl
from jax.experimental.pallas import tpu as pltpu
from jax.sharding import PartitionSpec as P

HEAD_DIM = 128
SOFTMAX_SCALE = HEAD_DIM ** -0.5
TRIPLE = 3 * HEAD_DIM
SP = 4
TP = 2
WIDTH = 128
PIECES = (4, 4, 1, 1, 1, 1, 1, 1, 1)
ALONE = 8
QUERIES = 256


def block_kernel(
    x_ref, doc_ref, wqkv_ref, wout_ref, y_ref,
    x_all, w_all, wo_all, o_all, o_mate, early_sums, qkv, doc_all,
    local_sem, x_send, x_recv, doc_send, doc_recv, w_send, w_recv, late_send, wo_mate_recv,
    wo_recv, wo_pass_recv, o_recv, of_recv, y_recv, last_recv, mate_send, mate_recv,
):
    me = lax.axis_index("sp")
    col = lax.axis_index("tp")
    rows, half = x_ref.shape
    depth = wqkv_ref.shape[0]
    heads = w_all.shape[0]
    cols = wout_ref.shape[1]
    chunks = cols // WIDTH
    last = chunks - 1
    other_col = 1 - col
    chip = me // 2
    core = lax.rem(me, 2)
    mate = chip * 2 + 1 - core
    across = (1 - chip) * 2 + core
    diagonal = (1 - chip) * 2 + 1 - core
    peers = (mate, across, diagonal)
    to_mate, to_across, to_diagonal, to_col = {"sp": mate}, {"sp": across}, {"sp": diagonal}, {"tp": other_col}
    to_peers = (to_mate, to_across, to_diagonal)
    to_col_mate = {"sp": mate, "tp": other_col}

    barrier = pltpu.get_barrier_semaphore()
    for where in (to_across, to_diagonal, to_col, to_col_mate, to_mate):
        pl.semaphore_signal(barrier, inc=1, device_id=where, device_id_type=pl.DeviceIdType.MESH)
    pl.semaphore_wait(barrier, 5)

    def remote(src, dst, send, recv, where):
        return pltpu.make_async_remote_copy(
            src_ref=src, dst_ref=dst, send_sem=send, recv_sem=recv,
            device_id=where, device_id_type=pl.DeviceIdType.MESH,
        )

    def take(sem, ref):
        remote(ref, ref, sem, sem, to_mate).wait_recv()

    def local(src, dst, i):
        return pltpu.make_async_copy(src, dst, local_sem.at[i])

    def at(i, size):
        return pl.ds(pl.multiple_of(i * size, size), size)

    def x_slot(c, s):
        return x_all.at[c, at(s, rows), :]

    def x_pass(c, s, recv, where):
        remote(x_slot(c, s), x_slot(c, s), x_send, x_recv.at[recv], where).start()

    own_x = x_slot(col, me)
    remote(x_ref, own_x, x_send, x_recv.at[0], to_across).start()
    remote(x_ref, own_x, x_send, x_recv.at[1], to_col).start()
    remote(x_ref, own_x, x_send, x_recv.at[3], to_mate).start()
    local(x_ref, own_x, 0).start()
    for where in to_peers:
        remote(doc_ref, doc_all.at[me], doc_send, doc_recv, where).start()
    local(doc_ref, doc_all.at[me], 1).start()

    def w_cols(owner, h):
        return wqkv_ref.at[:, at(owner * heads + h, TRIPLE)]

    def w_slot(h, s):
        return w_all.at[h, at(s, depth), :]

    def w_go(i, h):
        remote(w_cols(peers[i], h), w_slot(h, me), w_send, w_recv.at[h], to_peers[i]).start()

    for h in range(heads):
        if h < heads - 1:
            w_go(1, h)
            w_go(2, h)
        w_go(0, h)
        local(w_cols(me, h), w_slot(h, me), 0).start()
    own_wo = wo_all.at[at(me, depth), :]
    local(wout_ref, own_wo, 0).start()

    take(x_recv.at[1], x_slot(other_col, me))
    x_pass(other_col, me, 3, to_mate)
    take(x_recv.at[0], x_slot(col, across))
    x_pass(col, across, 2, to_col)
    x_pass(col, across, 3, to_mate)
    take(x_recv.at[2], x_slot(other_col, across))
    x_pass(other_col, across, 3, to_mate)
    mine = wo_all.at[pl.ds(0, (rows * half + heads * depth * TRIPLE + depth * cols) // cols), :]
    local(mine, mine, 0).wait()
    local(doc_ref, doc_all.at[me], 1).wait()
    take(doc_recv, doc_all.at[pl.ds(0, SP - 1)])
    take(x_recv.at[3], x_all.at[0])

    def wo_slot(s, j, count=1):
        return wo_all.at[at(s, depth), pl.ds(pl.multiple_of(j * WIDTH, WIDTH), count * WIDTH)]

    def wo_go(p):
        j, count = sum(PIECES[:p]), PIECES[p]
        src = wout_ref.at[:, pl.ds(j * WIDTH, count * WIDTH)]
        remote(src, wo_slot(me, j, count), late_send, wo_recv.at[p], to_across).start()

    def wo_pass(p, j, count):
        take(wo_recv.at[p], wo_slot(across, j, count))
        remote(wo_slot(across, j, count), wo_slot(across, j, count), late_send, wo_pass_recv.at[p], to_mate).start()

    def o_go(i, h):
        src = w_all.at[h, at(peers[i], rows), pl.ds(0, HEAD_DIM)]
        dst = o_all.at[col, me, :, at(h, HEAD_DIM)]
        remote(src, dst, late_send, o_recv.at[h], to_peers[i]).start()

    def o_pass(h):
        take(o_recv.at[h], w_all.at[0, pl.ds(0, rows), :])
        slot = o_all.at[col, :, :, at(h, HEAD_DIM)]
        remote(slot, slot, late_send, of_recv, to_col).start()

    def one_head(h, carry):
        take(w_recv.at[h], w_all.at[0, pl.ds(0, (SP - 1) * depth), :])

        def project(r, carry):
            tile = at(r, rows)
            total = jnp.dot(x_all[0, tile, :], w_all[h, :half, :], preferred_element_type=jnp.float32)
            total += jnp.dot(x_all[1, tile, :], w_all[h, half:, :], preferred_element_type=jnp.float32)
            qkv[tile, :] = total.astype(jnp.bfloat16)
            return carry

        lax.fori_loop(0, SP, project, 0)

        docs = jnp.concatenate([doc_all[s] for s in range(SP)], axis=1)
        per_block = rows // QUERIES

        def attend(r, carry):
            tile = at(r, QUERIES)
            scores = lax.dot_general(
                qkv[tile, :HEAD_DIM], qkv[:, HEAD_DIM:2 * HEAD_DIM], (((1,), (1,)), ((), ())),
                preferred_element_type=jnp.float32,
            ) * SOFTMAX_SCALE
            own = doc_all[r // per_block, :, at(lax.rem(r, per_block), QUERIES)]
            same = jnp.broadcast_to(own, (HEAD_DIM, QUERIES)).T[:, :1] == docs
            scores = jnp.where(same, scores, -jnp.inf)
            top = jnp.max(scores, axis=1, keepdims=True)
            weights = jnp.exp(scores - top)
            weights = weights * (1.0 / jnp.sum(weights, axis=1, keepdims=True))
            out = jnp.dot(weights.astype(jnp.bfloat16), qkv[:, 2 * HEAD_DIM:], preferred_element_type=jnp.float32)
            w_all[h, tile, :HEAD_DIM] = out.astype(jnp.bfloat16)
            return carry

        lax.fori_loop(0, SP * per_block, attend, 0)
        o_all[col, me, :, at(h, HEAD_DIM)] = w_all[h, at(me, rows), :HEAD_DIM]
        for i in (1, 2, 0):
            o_go(i, h)

        @pl.when(h == 0)
        def _():
            w_go(1, heads - 1)
            w_go(2, heads - 1)
            remote(wout_ref, own_wo, late_send, wo_mate_recv, to_mate).start()

        @pl.when(h == heads - 2)
        def _():
            wo_go(0)
            o_pass(0)

        return carry

    lax.fori_loop(0, heads, one_head, 0)
    for p in range(1, len(PIECES)):
        wo_go(p)

    take(wo_mate_recv, wo_all.at[pl.ds(0, depth), :])

    def last_slot(s, i, count=1):
        return wo_all.at[pl.ds(pl.multiple_of(s * depth + i * (depth // 2), depth // 2), count * (depth // 2)), at(last, WIDTH)]

    def last_go(k, src, owner, i, count=1):
        remote(src, last_slot(owner, i, count), mate_send, last_recv.at[k], to_across).start()

    @pl.when(core == 1)
    def _():
        last_go(0, last_slot(mate, 0, 2), mate, 0, 2)
        for i in range(2):
            last_go(1 + i, wout_ref.at[pl.ds(i * (depth // 2), depth // 2), at(last, WIDTH)], me, i)

    for h in range(1, heads):
        o_pass(h)

    span = rows // 2
    keep = at(col, span)
    give = at(other_col, span)

    def stage(j, k):
        return w_all.at[heads - 1, at(j, span), pl.ds(k * HEAD_DIM, WIDTH)]

    def y_slot(j):
        return y_ref.at[:, at(col * chunks + j, WIDTH)]

    def y_go(j, send=None):
        remote(stage(j, 1), y_slot(j), late_send if send is None else send, y_recv, to_col).start()

    def part(source, owner, piece, j, halves=(0, 1)):
        total = None
        for i in halves:
            term = jnp.dot(
                source[owner // 2, lax.rem(owner, 2) * 2 + i, piece, :], wo_all[at(owner * 2 + i, depth // 2), at(j, WIDTH)],
                preferred_element_type=jnp.float32,
            )
            total = term if total is None else total + term
        return total

    take(of_recv, o_all.at[0])

    @pl.when(core == 0)
    def _():
        remote(o_all, o_mate, mate_send, mate_recv.at[0], to_mate).start()

    take(doc_send, doc_all.at[pl.ds(0, SP - 1)])
    take(w_send, w_all.at[pl.ds(0, SP - 1)])

    blocks = ((o_mate, give), (o_all, give), (o_mate, keep), (o_all, keep))

    def finish(j, carry):
        @pl.when((j == last - 3) & (core == 1))
        def _():
            take(mate_recv.at[0], o_mate)
            for i, (source, piece) in enumerate(blocks):
                early_sums[i] = part(source, me, piece, last) + part(source, mate, piece, last)

        given = part(o_all, me, give, j) + part(o_all, mate, give, j)
        kept = part(o_all, me, keep, j) + part(o_all, mate, keep, j)

        @pl.when(j >= ALONE)
        def _():
            wo_pass(j - shift, j, 1)

        given += part(o_all, across, give, j)
        kept += part(o_all, across, keep, j)

        @pl.when(j >= ALONE)
        def _():
            take(wo_pass_recv.at[j - shift], wo_slot(diagonal, j))

        given += part(o_all, diagonal, give, j)
        stage(j, 1)[...] = given.astype(jnp.bfloat16)
        y_go(j)
        kept += part(o_all, diagonal, keep, j)
        y_slot(j)[...] = kept.astype(jnp.bfloat16)
        return carry

    wide = len(PIECES) - (last - ALONE)
    shift = ALONE - wide
    for p in range(wide):
        wo_pass(p, sum(PIECES[:p]), PIECES[p])
    for p in range(wide):
        take(wo_pass_recv.at[p], wo_slot(diagonal, sum(PIECES[:p]), PIECES[p]))
    lax.fori_loop(0, last, finish, 0)
    most = pl.ds(0, last * WIDTH)

    @pl.when(core == 1)
    def _():
        take(last_recv.at[0], last_slot(diagonal, 0, 2))
        totals = [early_sums[i] + part(source, diagonal, piece, last) for i, (source, piece) in enumerate(blocks)]
        take(last_recv.at[1], last_slot(across, 0))
        totals = [total + part(source, across, piece, last, (0,)) for total, (source, piece) in zip(totals, blocks)]
        take(last_recv.at[2], last_slot(across, 1))

        def whole(i):
            source, piece = blocks[i]
            return (totals[i] + part(source, across, piece, last, (1,))).astype(jnp.bfloat16)

        stage(0, 2)[...] = whole(0)
        to_col_mate_copy = remote(stage(0, 2), y_slot(last), mate_send, y_recv, to_col_mate)
        to_col_mate_copy.start()
        stage(last, 1)[...] = whole(1)
        y_go(last, mate_send)
        stage(1, 2)[...] = whole(2)
        kept_copy = remote(stage(1, 2), y_slot(last), mate_send, mate_recv.at[1], to_mate)
        kept_copy.start()
        y_slot(last)[...] = whole(3)
        take(mate_send, wo_all.at[pl.ds(0, (2 * depth + 3 * span) * WIDTH // cols), :])

    @pl.when(core == 0)
    def _():
        take(mate_send, wo_all.at[pl.ds(0, TP * rows), :])
        take(mate_recv.at[1], y_slot(last))

    take(x_send, wo_all.at[pl.ds(0, 7 * rows), :])
    late = 12 * rows * HEAD_DIM + 4 * rows * cols // SP + depth * cols + 2 * depth * last * WIDTH + span * last * WIDTH
    take(late_send, wo_all.at[pl.ds(0, late // cols), :])
    take(y_recv, y_ref.at[:, pl.ds(0, cols)])


def solution(mesh):
    def device_block(x_block, doc_block, wqkv_block, wout_block):
        rows, half = x_block.shape
        depth = wqkv_block.shape[0]
        heads = wqkv_block.shape[1] // (TRIPLE * SP)
        cols = wout_block.shape[1]
        bf16 = jnp.bfloat16
        dma = pltpu.SemaphoreType.DMA
        return pl.pallas_call(
            block_kernel,
            out_shape=pltpu.VMEM((rows // TP, cols * TP), bf16),
            in_specs=[pl.BlockSpec(memory_space=pl.ANY)] * 4,
            out_specs=pl.BlockSpec(memory_space=pltpu.VMEM),
            scratch_shapes=[
                pltpu.VMEM((TP, SP * rows, half), bf16),
                pltpu.VMEM((heads, SP * depth, TRIPLE), bf16),
                pltpu.VMEM((SP * depth, cols), bf16),
                pltpu.VMEM((TP, SP, rows, heads * HEAD_DIM), bf16),
                pltpu.VMEM((TP, SP, rows, heads * HEAD_DIM), bf16),
                pltpu.VMEM((4, rows // 2, WIDTH), jnp.float32),
                pltpu.VMEM((SP * rows, TRIPLE), bf16),
                pltpu.VMEM((SP, 1, rows), jnp.int32),
                dma((2,)),
                dma,
                dma((4,)),
                dma,
                dma,
                dma,
                dma((heads,)),
                dma,
                dma,
                dma((len(PIECES),)),
                dma((len(PIECES),)),
                dma((heads,)),
                dma,
                dma,
                dma((3,)),
                dma,
                dma((2,)),
            ],
            compiler_params=pltpu.CompilerParams(
                collective_id=0, has_side_effects=True, vmem_limit_bytes=60 * 1024 * 1024,
            ),
            name="attention_block",
        )(x_block, doc_block.reshape(1, rows), wqkv_block, wout_block)

    return jax.shard_map(
        device_block,
        mesh=mesh,
        in_specs=(P(("dp", "sp"), "tp"), P(("dp", "sp")), P("sp", "tp"), P("sp", "tp")),
        out_specs=P(("dp", "sp", "tp"), None),
        check_vma=False,
    )
```
